128 devices in a mesh: band: 8 (over x, core), grid: 16 (over z, y).
Axes of the slice: x: 4, y: 4, z: 4, core: 2. Of those that a mesh axis runs over, the one named last changes fastest.
Arguments:
- orbitals: bfloat16 [32768, 2048], P('grid', 'band'), may hold values from -6 to 6
- projectors: bfloat16 [128, 8, 128], replicated, may hold values from -0.5 to 0.5
- sphere_start: int32 [128], replicated, may hold values from 0 to 1920, as said below
- proj_count: int32 [128], replicated, may hold values from 1 to 8
- owner_slab: int32 [128], replicated, may hold values from 0 to 15, as said below
- correlation_coef: float32 [128, 8, 8], replicated, as said below
Outputs:
- rotated: bfloat16 [32768, 2048], P(('grid', 'band'))
The draws below stay inside these ranges and needn't reach their ends.
Inputs may be any that keep to these rules, and one draw needn't show every extreme that they name: `sphere_start`: a multiple of 128. `owner_slab`: every slab owns exactly 8 atoms. `correlation_coef`: each atom's matrix is symmetric positive definite.
All inputs are finite; a program needn't handle non-finite values.
Results may differ from the reference program's by a relative error of at most 0.0049.
Values may be sent and summed in bfloat16 or wider, within the bound.
A program may use at most 128 MiB of HBM per device.

```python
import jax
import jax.numpy as jnp
from jax import lax

NB = 2048
SPH = 128
NPMAX = 8
A_SLAB = 8
G_SLAB = 2048
NG = 32768
NA = 128


def draw_owner_slab(key, part):
    order = jax.random.permutation(jax.random.fold_in(key, 11), NA)
    return (order // A_SLAB).astype(jnp.int32)


def draw_sphere_start(key, part):
    blocks = jax.random.randint(jax.random.fold_in(key, 12), (NA,), 0, G_SLAB // SPH)
    return (blocks * SPH).astype(jnp.int32)


def draw_correlation_coef(key, part):
    noise_key = jax.random.fold_in(key, 13)
    factor = jax.random.normal(noise_key, (NA, NPMAX, NPMAX), jnp.float32)
    square = jnp.einsum('aik,ajk->aij', factor, factor) / NPMAX
    square = square + 0.5 * jnp.eye(NPMAX, dtype=jnp.float32)[None, :, :]
    return (square / (NA * NPMAX)).astype(jnp.float32)


def touch_ends(values, stream_key, least, high):
    longest = values.shape.index(max(values.shape))
    spots = []
    for shift in (0, 1):
        where = [jax.random.randint(jax.random.fold_in(stream_key, axis), (), 0, length) for axis, length in enumerate(values.shape)]
        where[longest] = (where[longest] + shift) % values.shape[longest]
        spots.append(tuple(where))
    return values.at[spots[0]].set(least).at[spots[1]].set(high)


def shard_levels(stream_key, dims, pieces, low, high):
    loudness, own = 1.0, jax.random.fold_in(stream_key, 6)
    for position, blocks in pieces:
        heights = jnp.exp(jax.random.uniform(jax.random.fold_in(own, position), (blocks,), jnp.float32, low / len(pieces), high / len(pieces)))
        loudness = loudness * jnp.repeat(heights, dims[position] // blocks).reshape([-1 if axis == position else 1 for axis in range(len(dims))])
    return loudness


def centred(own_key, extent, width, bound, shards=(), kind=jnp.bfloat16):
    values = width * jax.random.normal(own_key, extent, jnp.float32)
    if shards:
        values = values * shard_levels(own_key, extent, shards, -0.22, 0.18)
    return jnp.clip(values, -bound, bound).astype(kind)


def setup_inputs(seed: int = 0) -> dict:
    key_of = jax.random.split(jax.random.key(seed), 7)
    orbitals = centred(key_of[0], (NG, NB), 1.0, 6.0, ((0, 16), (1, 8)))
    projectors = centred(key_of[1], (NA, NPMAX, SPH), SPH ** -0.5, 0.5)
    sphere_start = draw_sphere_start(jax.random.fold_in(key_of[6], 71), 0)
    proj_count = touch_ends(jax.random.randint(key_of[3], (NA,), 1, NPMAX + 1), jax.random.fold_in(key_of[3], 1), 1, NPMAX).astype(jnp.int32)
    owner_slab = draw_owner_slab(jax.random.fold_in(key_of[6], 71), 0)
    correlation_coef = draw_correlation_coef(jax.random.fold_in(key_of[6], 71), 0)
    return {"orbitals": orbitals, "projectors": projectors, "sphere_start": sphere_start, "proj_count": proj_count, "owner_slab": owner_slab, "correlation_coef": correlation_coef}


def inverse_factor(matrix):
    order = matrix.shape[0]
    if order <= 512 or order % 2 != 0:
        lower = jnp.linalg.cholesky(matrix)
        identity = jnp.eye(order, dtype=matrix.dtype)
        return lax.linalg.triangular_solve(lower, identity, left_side=True, lower=True)
    half = order // 2
    upper_inv = inverse_factor(matrix[:half, :half])
    below = jnp.dot(matrix[half:, :half], upper_inv.T, precision=lax.Precision.HIGHEST)
    schur = matrix[half:, half:] - jnp.dot(below, below.T, precision=lax.Precision.HIGHEST)
    lower_inv = inverse_factor(schur)
    corner = -jnp.dot(lower_inv, jnp.dot(below, upper_inv, precision=lax.Precision.HIGHEST), precision=lax.Precision.HIGHEST)
    top = jnp.concatenate([upper_inv, jnp.zeros((half, order - half), matrix.dtype)], axis=1)
    bottom = jnp.concatenate([corner, lower_inv], axis=1)
    return jnp.concatenate([top, bottom], axis=0)

def reference(orbitals, projectors, sphere_start, proj_count, owner_slab, correlation_coef):
    total_rows = orbitals.shape[0]
    bands = orbitals.shape[1]
    gram = jnp.dot(orbitals.T.astype(jnp.float32), orbitals.astype(jnp.float32), preferred_element_type=jnp.float32) * (1.0 / total_rows)
    starts = (owner_slab * G_SLAB + sphere_start).astype(jnp.int32)

    def one_atom(packed):
        weights, start, number, coefs = packed
        sphere_rows = lax.dynamic_slice_in_dim(orbitals, start, SPH, 0)
        correlations = jnp.dot(weights.astype(jnp.float32), sphere_rows.astype(jnp.float32), preferred_element_type=jnp.float32)
        active = jnp.arange(NPMAX) < number
        correlations = jnp.where(active[:, None], correlations, jnp.zeros_like(correlations))
        weighted = jnp.dot(coefs, correlations, precision=lax.Precision.HIGHEST)
        return (correlations, weighted)
    correlations, weighted = lax.map(one_atom, (projectors, starts, proj_count, correlation_coef))
    paw = jnp.dot(weighted.reshape(-1, bands).T, correlations.reshape(-1, bands), precision=lax.Precision.HIGHEST)
    metric = gram + paw
    inverse = inverse_factor(metric).astype(jnp.bfloat16)
    return jnp.dot(orbitals.astype(jnp.float32), inverse.T.astype(jnp.float32), preferred_element_type=jnp.float32).astype(jnp.bfloat16)
```

```python
import jax
import jax.numpy as jnp
from jax import lax
from jax.experimental import pallas as pl
from jax.experimental.pallas import tpu as pltpu
from jax.sharding import PartitionSpec as P

F32 = jnp.float32
BF = jnp.bfloat16
SPH = 128
NPMAX = 8
A_SLAB = 8


def chol_inv_128(a_ref, w_ref):
    n=128; T=16
    A=[a_ref[8*t:8*t+8,:] for t in range(T)]
    lane=lax.broadcasted_iota(jnp.int32,(8,128),1)
    sub=lax.broadcasted_iota(jnp.int32,(8,128),0)
    W=[jnp.where(lane==sub+8*t,1.0,0.0).astype(F32) for t in range(T)]
    for g in range(T):
        C=[[jnp.broadcast_to(A[t][:,8*g+c:8*g+c+1],(8,128)) for t in range(T)] if True else None for c in range(0)]
        C=[{t:jnp.broadcast_to(A[t][:,8*g+c:8*g+c+1],(8,128)) for t in range(g,T)} for c in range(8)]
        S=jnp.ones((8,128),F32)
        for c in range(8):
            d=jnp.broadcast_to(C[c][g][c:c+1,:],(8,128))
            S=jnp.where(sub==c,d,S)
            inv=1.0/d
            Cc=dict(C[c])
            if c<7:
                Cc[g]=jnp.where(sub>c,C[c][g],0.0)
            ra=jnp.broadcast_to(A[g][c:c+1,:],(8,128))*inv
            rw=jnp.broadcast_to(W[g][c:c+1,:],(8,128))*inv
            rc={j:jnp.broadcast_to(C[j][g][c:c+1,:],(8,128))*inv for j in range(c+1,8)}
            t0=g if c<7 else g+1
            for t in range(t0,T):
                for j in range(c+1,8):
                    C[j][t]=C[j][t]-Cc[t]*rc[j]
                A[t]=A[t]-Cc[t]*ra
                W[t]=W[t]-Cc[t]*rw
        w_ref[8*g:8*g+8,:]=W[g]*lax.rsqrt(S)


B=256
HI=lax.Precision.HIGHEST
def splt(x):
    h=x.astype(BF); return h,(x-h.astype(F32)).astype(BF)
def nt(a,b,prec=None):
    return lax.dot_general(a,b,(((1,),(1,)),((),())),preferred_element_type=F32,precision=prec)
def tn(a,b,prec=None):
    return lax.dot_general(a,b,(((0,),(0,)),((),())),preferred_element_type=F32,precision=prec)
def nn(a,b,prec=None):
    return lax.dot_general(a,b,(((1,),(0,)),((),())),preferred_element_type=F32,precision=prec)

def fac_kernel(m_ref, x_ref, o_ref, T, UT, U, Wd, Ws, Wt, sem):
    NBK=8
    cps=[]
    for i in range(NBK):
        for c in range(i,NBK):
            cp=pltpu.make_async_copy(m_ref.at[pl.ds(B*i,B),pl.ds(B*c,B)],T.at[i,c],sem.at[i])
            cp.start(); cps.append((i,cp))
    for c in range(NBK):
        T[8,c]=x_ref[:,B*c:B*c+B].astype(F32)
    for i,cp in cps: cp.wait()
    Wd[...]=jnp.zeros((B,B),F32)
    def step(j,_):
        D=T.at[j,j]
        chol_inv_128(D.at[pl.ds(0,128),pl.ds(0,128)],Wd.at[pl.ds(0,128),pl.ds(0,128)])
        W1=Wd[0:128,0:128]
        u12=nn(W1,T[j,j,0:128,128:256],HI)
        T[j,j,128:256,128:256]=T[j,j,128:256,128:256]-tn(u12,u12,HI)
        chol_inv_128(D.at[pl.ds(128,128),pl.ds(128,128)],Wd.at[pl.ds(128,128),pl.ds(128,128)])
        W2=Wd[128:256,128:256]
        Wd[128:256,0:128]=-nn(W2,tn(u12,W1,HI),HI)
        h,l=splt(Wd[...])
        Ws[:,0:B]=h; Ws[:,B:2*B]=h; Ws[:,2*B:3*B]=l
        Wt[:,0:B]=h; Wt[:,B:2*B]=l; Wt[:,2*B:3*B]=h
        h,l=splt(T[8,j])
        r=nt(jnp.concatenate([h,h,l],axis=1),Wt[...])
        h=r.astype(BF)
        o_ref[j]=h
        l=(r-h.astype(F32)).astype(BF)
        UT[8,:,0:B]=h; UT[8,:,B:2*B]=h; UT[8,:,2*B:3*B]=l
        def pan(c,_):
            h,l=splt(T[j,c])
            u=nn(Ws[...],jnp.concatenate([h,l,h],axis=0))
            h,l=splt(u)
            U[c,0:B,:]=h; U[c,B:2*B,:]=l; U[c,2*B:3*B,:]=h
            h,l=splt(u.T)
            UT[c,:,0:B]=h; UT[c,:,B:2*B]=h; UT[c,:,2*B:3*B]=l
            return 0
        lax.fori_loop(j+1,NBK,pan,0)
        def row(i,_):
            def col(c,_):
                T[i,c]=T[i,c]-nn(UT[i],U[c])
                return 0
            lax.fori_loop(jnp.where(i==8,j+1,i),NBK,col,0)
            return 0
        lax.fori_loop(j+1,NBK+1,row,0)
        return 0
    lax.fori_loop(0,NBK,step,0)

def factor_rotate(metric, mine):
    o=pl.pallas_call(fac_kernel,out_shape=jax.ShapeDtypeStruct((8,B,B),BF),
      in_specs=[pl.BlockSpec(memory_space=pltpu.HBM),pl.BlockSpec(memory_space=pltpu.VMEM)],
      out_specs=pl.BlockSpec(memory_space=pltpu.VMEM),
      scratch_shapes=[pltpu.VMEM((9,8,B,B),F32),pltpu.VMEM((9,B,3*B),BF),pltpu.VMEM((8,3*B,B),BF),
         pltpu.VMEM((B,B),F32),pltpu.VMEM((B,3*B),BF),pltpu.VMEM((B,3*B),BF),pltpu.SemaphoreType.DMA((8,))],
      compiler_params=pltpu.CompilerParams(vmem_limit_bytes=56*2**20))(metric,mine)
    return o.transpose(1,0,2).reshape(B,8*B)


def slab_atoms(owner_slab, slab):
    atoms = owner_slab.shape[0]
    keyed = jnp.where(owner_slab == slab, 0, 1) * atoms + jnp.arange(atoms, dtype=jnp.int32)
    return jnp.argsort(keyed, stable=True)[:A_SLAB]


def atom_terms(source, weights, starts, counts, coefs, valid):

    def take_rows(offset):
        return lax.dynamic_slice_in_dim(source, offset, SPH, 0)

    sphere_rows = jax.vmap(take_rows)(starts)
    correlations = jnp.einsum(
        "aij,ajn->ain", weights, sphere_rows, preferred_element_type=jnp.float32
    )
    active = (jnp.arange(NPMAX)[None, :] < counts[:, None]) & valid[:, None]
    correlations = jnp.where(active[:, :, None], correlations, jnp.zeros_like(correlations))
    weighted = jnp.einsum("aij,ajn->ain", coefs, correlations, precision=lax.Precision.HIGHEST)
    return (correlations, weighted)


def shards(orbitals, projectors, sphere_start, proj_count, owner_slab, correlation_coef):
    band_index = lax.axis_index("band")
    slab = lax.axis_index("grid")
    nbands = lax.axis_size("band")
    total_rows = orbitals.shape[0] * lax.axis_size("grid")
    chosen = slab_atoms(owner_slab, slab)
    weights = projectors[chosen]
    counts = proj_count[chosen]
    coefs = correlation_coef[chosen]
    gathered = lax.all_gather(orbitals, "band", axis=1, tiled=True)
    width = orbitals.shape[1]
    width_all = gathered.shape[1]
    gram_panel = jnp.dot(orbitals.T, gathered, preferred_element_type=jnp.float32) * (
        1.0 / total_rows
    )
    valid = jnp.ones((A_SLAB,), dtype=bool)
    correlations, weighted = atom_terms(
        gathered, weights, sphere_start[chosen], counts, coefs, valid
    )
    panel_weighted = lax.dynamic_slice_in_dim(weighted, band_index * width, width, 2)
    paw = jnp.dot(
        panel_weighted.reshape(-1, width).T,
        correlations.reshape(-1, width_all),
        precision=lax.Precision.HIGHEST,
    )
    panel_total = lax.psum(gram_panel + paw, "grid")
    metric = lax.all_gather(panel_total, "band", axis=0, tiled=True)
    height = orbitals.shape[0] // nbands
    mine = lax.dynamic_slice_in_dim(gathered, band_index * height, height, 0)
    return factor_rotate(metric, mine)


def solution(mesh):
    in_specs = (P("grid", "band"), P(), P(), P(), P(), P())
    out_specs = P(("grid", "band"), None)
    return jax.shard_map(shards, mesh=mesh, in_specs=in_specs, out_specs=out_specs, check_vma=False)
```

```python
import jax
import jax.numpy as jnp
from jax import lax
from jax.experimental import pallas as pl
from jax.experimental.pallas import tpu as pltpu
from jax.sharding import PartitionSpec as P

F32 = jnp.float32
BF = jnp.bfloat16
SPH = 128
NPMAX = 8
A_SLAB = 8


def chol_inv_128(a_ref, w_ref):
    n=128; T=16
    A=[a_ref[8*t:8*t+8,:] for t in range(T)]
    lane=lax.broadcasted_iota(jnp.int32,(8,128),1)
    sub=lax.broadcasted_iota(jnp.int32,(8,128),0)
    W=[jnp.where(lane==sub+8*t,1.0,0.0).astype(F32) for t in range(T)]
    for g in range(T):
        C=[[jnp.broadcast_to(A[t][:,8*g+c:8*g+c+1],(8,128)) for t in range(T)] if True else None for c in range(0)]
        C=[{t:jnp.broadcast_to(A[t][:,8*g+c:8*g+c+1],(8,128)) for t in range(g,T)} for c in range(8)]
        S=jnp.ones((8,128),F32)
        for c in range(8):
            d=jnp.broadcast_to(C[c][g][c:c+1,:],(8,128))
            S=jnp.where(sub==c,d,S)
            inv=1.0/d
            Cc=dict(C[c])
            if c<7:
                Cc[g]=jnp.where(sub>c,C[c][g],0.0)
            ra=jnp.broadcast_to(A[g][c:c+1,:],(8,128))*inv
            rw=jnp.broadcast_to(W[g][c:c+1,:],(8,128))*inv
            rc={j:jnp.broadcast_to(C[j][g][c:c+1,:],(8,128))*inv for j in range(c+1,8)}
            t0=g if c<7 else g+1
            for t in range(t0,T):
                for j in range(c+1,8):
                    C[j][t]=C[j][t]-Cc[t]*rc[j]
                A[t]=A[t]-Cc[t]*ra
                W[t]=W[t]-Cc[t]*rw
        w_ref[8*g:8*g+8,:]=W[g]*lax.rsqrt(S)


B=256
HI=lax.Precision.HIGHEST
def splt(x):
    h=x.astype(BF); return h,(x-h.astype(F32)).astype(BF)
def nt(a,b,prec=None):
    return lax.dot_general(a,b,(((1,),(1,)),((),())),preferred_element_type=F32,precision=prec)
def tn(a,b,prec=None):
    return lax.dot_general(a,b,(((0,),(0,)),((),())),preferred_element_type=F32,precision=prec)
def nn(a,b,prec=None):
    return lax.dot_general(a,b,(((1,),(0,)),((),())),preferred_element_type=F32,precision=prec)

def fac_kernel(m_ref, x_ref, o_ref, T, UT, U, Wd, Ws, Wt, sem):
    NBK=8
    cps=[]
    for i in range(NBK):
        for c in range(i,NBK):
            t=PAIRS.index((i,c))
            for h in range(2):
                k=len(cps)
                cp=pltpu.make_async_copy(m_ref.at[t//18,pl.ds((t%18)*512+256*h,256),:],T.at[i,c,:,pl.ds(128*h,128)],sem.at[k])
                cp.start(); cps.append(cp)
    for c in range(NBK):
        T[8,c]=x_ref[c].astype(F32)
    for cp in cps: cp.wait()
    Wd[...]=jnp.zeros((B,B),F32)
    def step(j,_):
        D=T.at[j,j]
        chol_inv_128(D.at[pl.ds(0,128),pl.ds(0,128)],Wd.at[pl.ds(0,128),pl.ds(0,128)])
        W1=Wd[0:128,0:128]
        u12=nn(W1,T[j,j,0:128,128:256],HI)
        T[j,j,128:256,128:256]=T[j,j,128:256,128:256]-tn(u12,u12,HI)
        chol_inv_128(D.at[pl.ds(128,128),pl.ds(128,128)],Wd.at[pl.ds(128,128),pl.ds(128,128)])
        W2=Wd[128:256,128:256]
        Wd[128:256,0:128]=-nn(W2,tn(u12,W1,HI),HI)
        h,l=splt(Wd[...])
        Ws[:,0:B]=h; Ws[:,B:2*B]=h; Ws[:,2*B:3*B]=l
        Wt[:,0:B]=h; Wt[:,B:2*B]=l; Wt[:,2*B:3*B]=h
        h,l=splt(T[8,j])
        r=nt(jnp.concatenate([h,h,l],axis=1),Wt[...])
        h=r.astype(BF)
        o_ref[j]=h
        l=(r-h.astype(F32)).astype(BF)
        UT[8,:,0:B]=h; UT[8,:,B:2*B]=h; UT[8,:,2*B:3*B]=l
        def pan(c,_):
            h,l=splt(T[j,c])
            u=nn(Ws[...],jnp.concatenate([h,l,h],axis=0))
            h,l=splt(u)
            U[c,0:B,:]=h; U[c,B:2*B,:]=l; U[c,2*B:3*B,:]=h
            h,l=splt(u.T)
            UT[c,:,0:B]=h; UT[c,:,B:2*B]=h; UT[c,:,2*B:3*B]=l
            return 0
        lax.fori_loop(j+1,NBK,pan,0)
        def row(i,_):
            def col(c,_):
                T[i,c]=T[i,c]-nn(UT[i],U[c])
                return 0
            lax.fori_loop(jnp.where(i==8,j+1,i),NBK,col,0)
            return 0
        lax.fori_loop(j+1,NBK+1,row,0)
        return 0
    lax.fori_loop(0,NBK,step,0)

def factor_rotate(metric, mine):
    o=pl.pallas_call(fac_kernel,out_shape=jax.ShapeDtypeStruct((8,B,B),BF),
      in_specs=[pl.BlockSpec(memory_space=pltpu.HBM),pl.BlockSpec(memory_space=pltpu.VMEM)],
      out_specs=pl.BlockSpec(memory_space=pltpu.VMEM),
      scratch_shapes=[pltpu.VMEM((9,8,B,B),F32),pltpu.VMEM((9,B,3*B),BF),pltpu.VMEM((8,3*B,B),BF),
         pltpu.VMEM((B,B),F32),pltpu.VMEM((B,3*B),BF),pltpu.VMEM((B,3*B),BF),pltpu.SemaphoreType.DMA((72,))],
      compiler_params=pltpu.CompilerParams(vmem_limit_bytes=56*2**20))(metric,mine)
    return o.transpose(1,0,2).reshape(B,8*B)


MESH = pl.DeviceIdType.MESH
XDT = F32


def barrier(peers):
    sem = pltpu.get_barrier_semaphore()
    for peer in peers:
        pl.semaphore_signal(sem, inc=1, device_id=peer, device_id_type=MESH)
    pl.semaphore_wait(sem, len(peers))


def swap_kernel(x_ref, o_ref, ssem, rsem, fsem, gsem):
    me = lax.axis_index("band")
    core = lax.rem(me, 2)
    mate = me + 1 - 2 * core
    barrier([{"band": lax.rem(me + d, 8)} for d in range(1, 8)])
    sends = []
    for d in (4, 3, 5, 2, 6, 1, 7):
        peer = lax.rem(me + d, 8)
        cp = pltpu.make_async_remote_copy(
            src_ref=x_ref.at[pl.ds(pl.multiple_of(256 * peer, 256), 256), :],
            dst_ref=o_ref.at[lax.rem(peer, 2), me],
            send_sem=ssem.at[d - 1], recv_sem=rsem.at[d - 1],
            device_id={"band": peer}, device_id_type=MESH)
        cp.start()
        sends.append(cp)
    own = x_ref.at[pl.ds(pl.multiple_of(256 * me, 256), 256), :]
    cp0 = pltpu.make_async_remote_copy(
        src_ref=own, dst_ref=o_ref.at[core, me], send_sem=fsem.at[7], recv_sem=gsem.at[7],
        device_id={"band": mate}, device_id_type=MESH)
    cp0.start()
    lsem = ssem.at[7]
    loc = pltpu.make_async_copy(own, o_ref.at[core, me], lsem)
    loc.start()
    fwd = [cp0]
    for d, s in zip((1, 7, 2, 6, 3, 5, 4), (5, 6, 3, 4, 1, 2, 0)):
        sends[s].wait_recv()
        k = lax.rem(me + 8 - d, 8)
        cp = pltpu.make_async_remote_copy(
            src_ref=o_ref.at[core, k], dst_ref=o_ref.at[core, k],
            send_sem=fsem.at[d - 1], recv_sem=gsem.at[d - 1],
            device_id={"band": mate}, device_id_type=MESH)
        cp.start()
        fwd.append(cp)
    loc.wait()
    for cp in fwd:
        cp.wait()
    for cp in sends:
        cp.wait_send()


def swap(x):
    return pl.pallas_call(
        swap_kernel, out_shape=jax.ShapeDtypeStruct((2, 8, 256, 256), BF),
        in_specs=[pl.BlockSpec(memory_space=pltpu.VMEM)],
        out_specs=pl.BlockSpec(memory_space=pltpu.VMEM),
        scratch_shapes=[pltpu.SemaphoreType.DMA((8,))] * 4,
        compiler_params=pltpu.CompilerParams(collective_id=0, has_side_effects=True))(x)


def gram_kernel(p_tab, q_tab, x_ref, pm_ref, cb_ref, o_ref, L, R):
    scale = 1.0 / 32768
    for k in range(8):
        corr = nn(pm_ref[0], x_ref[0, k]) + nn(pm_ref[1], x_ref[1, k])
        wgt = nn(cb_ref[...], corr, HI)
        ch, cl = splt(corr)
        wh, wl = splt(wgt)
        R[k, 0:256, :] = x_ref[0, k]
        R[k, 256:512, :] = x_ref[1, k]
        R[k, 512:576, :] = ch
        R[k, 576:640, :] = cl
        R[k, 640:704, :] = ch
        lt = jnp.concatenate([x_ref[0, k].astype(F32) * scale, x_ref[1, k].astype(F32) * scale,
                              wh.astype(F32), wh.astype(F32), wl.astype(F32)], axis=0)
        L[k] = lt.T.astype(BF)

    def block(t, _):
        g = nn(L[p_tab[t]], R[q_tab[t]]).astype(XDT)
        at = pl.multiple_of(t * 512, 512)
        o_ref[pl.ds(at, 256), :] = g[:, 0:128]
        o_ref[pl.ds(at + 256, 256), :] = g[:, 128:256]
        return 0
    lax.fori_loop(0, 18, block, 0)


def gram(p_tab, q_tab, x, pm, cb):
    vm = pl.BlockSpec(memory_space=pltpu.VMEM)
    sm = pl.BlockSpec(memory_space=pltpu.SMEM)
    return pl.pallas_call(
        gram_kernel, out_shape=jax.ShapeDtypeStruct((9216, 128), XDT),
        in_specs=[sm, sm, vm, vm, vm], out_specs=vm,
        scratch_shapes=[pltpu.VMEM((8, 256, 704), BF), pltpu.VMEM((8, 704, 256), BF)],
        compiler_params=pltpu.CompilerParams(vmem_limit_bytes=40 * 2**20))(p_tab, q_tab, x, pm, cb)


def sum_kernel(p_ref, o_ref, r1, r2, r3, s1, s2, ssem, rsem, fsem, gsem):
    band, grid = lax.axis_index("band"), lax.axis_index("grid")
    x, core = lax.div(band, 2), lax.rem(band, 2)
    z, y = lax.div(grid, 4), lax.rem(grid, 4)
    at = {"x": x, "y": y, "z": z}

    def peer(axis, d):
        to = lax.rem(at[axis] + d, 4)
        return {"x": {"band": 2 * to + core}, "y": {"grid": 4 * z + to}, "z": {"grid": 4 * to + y}}[axis]

    orders = ("xyz", "yzx", "zxy")
    mate = {"band": band + 1 - 2 * core}
    barrier([peer(a, d) for a in "xyz" for d in (1, 2, 3)] + [mate])

    def rows(start, n):
        return pl.ds(pl.multiple_of(start, 16), n)

    pend = []

    def send(stage, k, d, src, dst):
        i = (stage * 3 + k) * 3 + d - 1
        cp = pltpu.make_async_remote_copy(
            src_ref=src, dst_ref=dst, send_sem=ssem.at[i], recv_sem=rsem.at[i],
            device_id=peer(orders[k][stage if stage < 3 else 5 - stage], d), device_id_type=MESH)
        cp.start()
        pend.append(cp)
        return cp

    live = {}
    for d in (2, 1, 3):
        for k in range(3):
            a = lax.rem(at[orders[k][0]] + d, 4)
            live[k, d] = send(0, k, d, p_ref.at[rows(k * 3072 + a * 768, 768), :], r1.at[k, d - 1])
    for k in range(3):
        for d in (1, 3, 2):
            live[k, d].wait_recv()
        a = at[orders[k][0]]
        tot = p_ref[rows(k * 3072 + a * 768, 768), :].astype(F32)
        for d in range(3):
            tot = tot + r1[k, d].astype(F32)
        s1[k] = tot.astype(XDT)
        for d in (2, 1, 3):
            b = lax.rem(at[orders[k][1]] + d, 4)
            live[k, d] = send(1, k, d, s1.at[k, rows(b * 192, 192), :], r2.at[k, d - 1])
    for k in range(3):
        for d in (1, 3, 2):
            live[k, d].wait_recv()
        b = at[orders[k][1]]
        tot = s1[k, rows(b * 192, 192), :].astype(F32)
        for d in range(3):
            tot = tot + r2[k, d].astype(F32)
        s2[k] = tot.astype(XDT)
        for d in (2, 1, 3):
            c = lax.rem(at[orders[k][2]] + d, 4)
            live[k, d] = send(2, k, d, s2.at[k, rows(c * 48, 48), :], r3.at[k, d - 1])
    base = {}
    for k in range(3):
        for d in (1, 3, 2):
            live[k, d].wait_recv()
        a, b, c = (at[v] for v in orders[k])
        tot = s2[k, rows(c * 48, 48), :].astype(F32)
        for d in range(3):
            tot = tot + r3[k, d].astype(F32)
        base[k] = (k * 3072 + a * 768, b * 192, c * 48)
        here = o_ref.at[core, rows(sum(base[k]), 48), :]
        o_ref[core, rows(sum(base[k]), 48), :] = tot.astype(XDT)
        for d in (2, 1, 3):
            live[k, d] = send(3, k, d, here, here)
    for k in range(3):
        for d in (1, 3, 2):
            live[k, d].wait_recv()
        here = o_ref.at[core, rows(base[k][0] + base[k][1], 192), :]
        for d in (2, 1, 3):
            live[k, d] = send(4, k, d, here, here)
    fwd = []

    def forward(k, d, a):
        blk = o_ref.at[core, rows(k * 3072 + a * 768, 768), :]
        cp = pltpu.make_async_remote_copy(
            src_ref=blk, dst_ref=blk, send_sem=fsem.at[k * 4 + d], recv_sem=gsem.at[k * 4 + d],
            device_id=mate, device_id_type=MESH)
        cp.start()
        fwd.append(cp)

    for k in range(3):
        for d in (1, 3, 2):
            live[k, d].wait_recv()
        here = o_ref.at[core, rows(base[k][0], 768), :]
        for d in (2, 1, 3):
            live[k, d] = send(5, k, d, here, here)
        forward(k, 0, at[orders[k][0]])
    for d in (1, 3, 2):
        for k in range(3):
            live[k, d].wait_recv()
            forward(k, d, lax.rem(at[orders[k][0]] + 4 - d, 4))
    for cp in fwd:
        cp.wait()
    for cp in pend:
        cp.wait_send()


def total(part):
    vm = pl.BlockSpec(memory_space=pltpu.VMEM)
    return pl.pallas_call(
        sum_kernel, out_shape=jax.ShapeDtypeStruct((2, 9216, 128), XDT),
        in_specs=[vm], out_specs=vm,
        scratch_shapes=[pltpu.VMEM((3, 3, 768, 128), XDT), pltpu.VMEM((3, 3, 192, 128), XDT),
                        pltpu.VMEM((3, 3, 48, 128), XDT), pltpu.VMEM((3, 768, 128), XDT),
                        pltpu.VMEM((3, 192, 128), XDT),
                        pltpu.SemaphoreType.DMA((54,)), pltpu.SemaphoreType.DMA((54,)),
                        pltpu.SemaphoreType.DMA((12,)), pltpu.SemaphoreType.DMA((12,))],
        compiler_params=pltpu.CompilerParams(collective_id=1, has_side_effects=True,
                                             vmem_limit_bytes=40 * 2**20))(part)


PAIRS = [(i, c) for i in range(8) for c in range(i, 8)]


def shards(orbitals, projectors, sphere_start, proj_count, owner_slab, correlation_coef):
    band = lax.axis_index("band")
    slab = lax.axis_index("grid")
    chip, core = band // 2, band % 2
    atoms = owner_slab.shape[0]
    mask = owner_slab == slab
    ids = jnp.arange(atoms, dtype=jnp.int32)
    rank = jnp.sum((ids[None, :] < ids[:, None]) & mask[None, :], axis=1, dtype=jnp.int32)
    pick = mask[None, :] & (rank[None, :] == jnp.arange(A_SLAB, dtype=jnp.int32)[:, None])
    starts = jnp.sum(jnp.where(pick, sphere_start[None, :], 0), axis=1)
    counts = jnp.sum(jnp.where(pick, proj_count[None, :], 0), axis=1)
    weights = jnp.dot(pick.astype(BF), projectors.reshape(atoms, NPMAX * SPH), preferred_element_type=F32)
    coefs = jnp.dot(pick.astype(F32), correlation_coef.reshape(atoms, NPMAX * NPMAX), precision=HI)
    active = jnp.arange(NPMAX, dtype=jnp.int32)[None, :] < counts[:, None]
    weights = jnp.where(active[:, :, None], weights.reshape(A_SLAB, NPMAX, SPH), 0.0).reshape(64, SPH)
    place = jnp.repeat(starts // SPH - chip * 4, NPMAX)
    pm = jnp.where(place[None, :, None, None] == jnp.arange(4, dtype=jnp.int32).reshape(2, 1, 2, 1),
                   weights[None, :, None, :], 0.0).reshape(2, 64, 256).astype(BF)
    eye = jnp.eye(A_SLAB, dtype=F32)
    cb = (eye[:, None, :, None] * coefs.reshape(A_SLAB, NPMAX, 1, NPMAX)).reshape(64, 64)
    p_all = jnp.asarray([p for p, _ in PAIRS], jnp.int32).reshape(2, 18)
    q_all = jnp.asarray([q for _, q in PAIRS], jnp.int32).reshape(2, 18)
    p_tab = jnp.where(core == 0, p_all[0], p_all[1])
    q_tab = jnp.where(core == 0, q_all[0], q_all[1])
    rows = swap(orbitals)
    part = gram(p_tab, q_tab, rows, pm, cb)
    metric = total(part)
    mine = lax.dynamic_index_in_dim(rows, core, 0, keepdims=False)
    return factor_rotate(metric, mine)


def solution(mesh):
    in_specs = (P("grid", "band"), P(), P(), P(), P(), P())
    out_specs = P(("grid", "band"), None)
    return jax.shard_map(shards, mesh=mesh, in_specs=in_specs, out_specs=out_specs, check_vma=False)
```

```python
import jax
import jax.numpy as jnp
from jax import lax
from jax.experimental import pallas as pl
from jax.experimental.pallas import tpu as pltpu
from jax.sharding import PartitionSpec as P

F32 = jnp.float32
BF = jnp.bfloat16
SPH = 128
NPMAX = 8
A_SLAB = 8


def chol_inv_128(a_ref, w_ref, extra=None):
    T=16
    full=(8,128)
    lane=lax.broadcasted_iota(jnp.int32,full,1)
    sub=lax.broadcasted_iota(jnp.int32,full,0)
    spread=lambda v,k: jnp.broadcast_to(v[:,k:k+1],full)
    row=lambda v,c: jnp.broadcast_to(v[c:c+1,:],full)
    A=[a_ref[8*t:8*t+8,:] for t in range(T)]
    W=[jnp.where(lane==sub+8*t,1.0,0.0).astype(F32) for t in range(T)]
    zero=jnp.minimum(jnp.abs(A[0]),0.0)
    D=[spread(A[0],c)+zero for c in range(8)]
    for g in range(T):
        C={t:[spread(A[t],8*g+c) for c in range(8)] for t in range(g+1,T)}
        if g+1<T:
            N=[spread(A[g+1],8*g+8+c) for c in range(8)]
        inv=[];ra=[];rw=[];rc=[]
        S=jnp.ones(full,F32)
        for c in range(8):
            d=row(D[c],c)
            S=jnp.where(sub==c,d,S)
            inv.append(1.0/d)
            ra.append(row(A[g],c)*inv[c])
            rw.append(row(W[g],c)*inv[c])
            rc.append({j:row(D[j],c)*inv[c] for j in range(c+1,8)})
            if c<7:
                m=jnp.where(sub>c,D[c],0.0)
                for j in range(c+1,8):
                    D[j]=D[j]-m*rc[c][j]
                A[g]=A[g]-m*ra[c]
                W[g]=W[g]-m*rw[c]
        w_ref[8*g:8*g+8,:]=W[g]*lax.rsqrt(S)
        if extra is not None: extra(g)
        for t in range(g+1,T):
            for c in range(8):
                for j in range(c+1,8):
                    C[t][j]=C[t][j]-C[t][c]*rc[c][j]
                A[t]=A[t]-C[t][c]*ra[c]
                W[t]=W[t]-C[t][c]*rw[c]
            if t==g+1:
                for c in range(8):
                    e=C[t][c]*inv[c]
                    for k in range(8):
                        N[k]=N[k]-C[t][c]*row(e,k)
                D=N


PAIRS = [(i, c) for i in range(8) for c in range(i, 8)]
HI=lax.Precision.HIGHEST
B=256
def splt(x):
    h=x.astype(BF); return h,(x-h.astype(F32)).astype(BF)
def nt(a,b,prec=None):
    return lax.dot_general(a,b,(((1,),(1,)),((),())),preferred_element_type=F32,precision=prec)
def nn(a,b,prec=None):
    return lax.dot_general(a,b,(((1,),(0,)),((),())),preferred_element_type=F32,precision=prec)
def left(x):
    h,l=splt(x); return jnp.concatenate([h,h,l],axis=1)
def right(x):
    h,l=splt(x); return jnp.concatenate([h,l,h],axis=0)

NBK=8
def later_tiles():
    rows,cols=[],[]
    for j in range(NBK):
        todo=[(i,c) for i in range(j+1,NBK) for c in range(i,NBK)]+[(8,c) for c in range(j+1,NBK)] if j else []
        assert len(todo)<=32
        todo=todo+[(7,0)]*(32-len(todo))
        rows+=[i for i,_ in todo]; cols+=[c for _,c in todo]
    return rows,cols

def fac_kernel(core_ref, ti_ref, tc_ref, m_ref, x_ref, o_ref, T, UT, U, Wd, Ws, Wt):
    core=core_ref[0]
    for t,(i,c) in enumerate(PAIRS):
        for h in range(2):
            T[i,c,:,128*h:128*h+128]=m_ref[t//18,(t%18)*512+256*h:(t%18)*512+256*h+256,:].astype(F32)
    for c in range(NBK):
        T[8,c]=x_ref[core,c].astype(F32)
    Wd[...]=jnp.zeros((B,B),F32)
    UT[7]=jnp.zeros((B,3*B),BF); U[0]=jnp.zeros((3*B,B),BF); T[7,0]=jnp.zeros((B,B),F32)
    def tile(i,c):
        T[i,c]=T[i,c]-nn(UT[i],U[c])
    def step(j,_):
        def slot(s):
            k=j*32+s
            tile(ti_ref[k],tc_ref[k])
        D=T.at[j,j]
        chol_inv_128(D.at[pl.ds(0,128),pl.ds(0,128)],Wd.at[pl.ds(0,128),pl.ds(0,128)],lambda g: slot(g))
        W1=Wd[0:128,0:128]
        u12=nn(left(W1),right(T[j,j,0:128,128:256]))
        l21=left(u12.T)
        T[j,j,128:256,128:256]=T[j,j,128:256,128:256]-nn(l21,right(u12))
        V=nn(l21,right(W1))
        chol_inv_128(D.at[pl.ds(128,128),pl.ds(128,128)],Wd.at[pl.ds(128,128),pl.ds(128,128)],lambda g: slot(16+g))
        W2=Wd[128:256,128:256]
        Wd[128:256,0:128]=-nn(left(W2),right(V))
        h,l=splt(Wd[...])
        Ws[:,0:B]=h; Ws[:,B:2*B]=h; Ws[:,2*B:3*B]=l
        Wt[:,0:B]=h; Wt[:,B:2*B]=l; Wt[:,2*B:3*B]=h
        r=nt(left(T[8,j]),Wt[...])
        h=r.astype(BF)
        o_ref[:,pl.ds(pl.multiple_of(j*B,B),B)]=h
        l=(r-h.astype(F32)).astype(BF)
        UT[8,:,0:B]=h; UT[8,:,B:2*B]=h; UT[8,:,2*B:3*B]=l
        def pan(c,_):
            u=nn(Ws[...],right(T[j,c]))
            h,l=splt(u)
            U[c,0:B,:]=h; U[c,B:2*B,:]=l; U[c,2*B:3*B,:]=h
            UT[c]=left(u.T)
            return 0
        lax.fori_loop(j+1,NBK,pan,0)
        def urgent(c,_):
            tile(j+1,c)
            return 0
        lax.fori_loop(j+1,NBK,urgent,0)
        @pl.when(j<NBK-1)
        def _():
            tile(8,j+1)
        return 0
    lax.fori_loop(0,NBK,step,0)

def factor_rotate(core, metric, rows):
    vm=pl.BlockSpec(memory_space=pltpu.VMEM); sm=pl.BlockSpec(memory_space=pltpu.SMEM)
    ti,tc=later_tiles()
    return pl.pallas_call(fac_kernel,out_shape=jax.ShapeDtypeStruct((B,8*B),BF),
      in_specs=[sm,sm,sm,vm,vm], out_specs=vm,
      scratch_shapes=[pltpu.VMEM((9,8,B,B),F32),pltpu.VMEM((9,B,3*B),BF),pltpu.VMEM((8,3*B,B),BF),
         pltpu.VMEM((B,B),F32),pltpu.VMEM((B,3*B),BF),pltpu.VMEM((B,3*B),BF)],
      compiler_params=pltpu.CompilerParams(vmem_limit_bytes=56*2**20))(
        core.reshape(1),jnp.asarray(ti,jnp.int32),jnp.asarray(tc,jnp.int32),metric,rows)


MESH = pl.DeviceIdType.MESH
XDT = F32


def barrier(peers):
    sem = pltpu.get_barrier_semaphore()
    for peer in peers:
        pl.semaphore_signal(sem, inc=1, device_id=peer, device_id_type=MESH)
    pl.semaphore_wait(sem, len(peers))


def swap_kernel(x_ref, o_ref, ssem, rsem, fsem, gsem):
    me = lax.axis_index("band")
    core = lax.rem(me, 2)
    mate = me + 1 - 2 * core
    barrier([{"band": lax.rem(me + d, 8)} for d in range(1, 8)])
    sends = []
    for d in (4, 3, 5, 2, 6, 1, 7):
        peer = lax.rem(me + d, 8)
        cp = pltpu.make_async_remote_copy(
            src_ref=x_ref.at[pl.ds(pl.multiple_of(256 * peer, 256), 256), :],
            dst_ref=o_ref.at[lax.rem(peer, 2), me],
            send_sem=ssem.at[d - 1], recv_sem=rsem.at[d - 1],
            device_id={"band": peer}, device_id_type=MESH)
        cp.start()
        sends.append(cp)
    own = x_ref.at[pl.ds(pl.multiple_of(256 * me, 256), 256), :]
    cp0 = pltpu.make_async_remote_copy(
        src_ref=own, dst_ref=o_ref.at[core, me], send_sem=fsem.at[7], recv_sem=gsem.at[7],
        device_id={"band": mate}, device_id_type=MESH)
    cp0.start()
    lsem = ssem.at[7]
    loc = pltpu.make_async_copy(own, o_ref.at[core, me], lsem)
    loc.start()
    fwd = [cp0]
    for d, s in zip((1, 7, 2, 6, 3, 5, 4), (5, 6, 3, 4, 1, 2, 0)):
        sends[s].wait_recv()
        k = lax.rem(me + 8 - d, 8)
        cp = pltpu.make_async_remote_copy(
            src_ref=o_ref.at[core, k], dst_ref=o_ref.at[core, k],
            send_sem=fsem.at[d - 1], recv_sem=gsem.at[d - 1],
            device_id={"band": mate}, device_id_type=MESH)
        cp.start()
        fwd.append(cp)
    loc.wait()
    for cp in fwd:
        cp.wait()
    for cp in sends:
        cp.wait_send()


def swap(x):
    return pl.pallas_call(
        swap_kernel, out_shape=jax.ShapeDtypeStruct((2, 8, 256, 256), BF),
        in_specs=[pl.BlockSpec(memory_space=pltpu.VMEM)],
        out_specs=pl.BlockSpec(memory_space=pltpu.VMEM),
        scratch_shapes=[pltpu.SemaphoreType.DMA((8,))] * 4,
        compiler_params=pltpu.CompilerParams(collective_id=0, has_side_effects=True))(x)


def gram_kernel(p_tab, q_tab, x_ref, pm_ref, cb_ref, o_ref, L, R):
    scale = 1.0 / 32768
    for k in range(8):
        corr = nn(pm_ref[0], x_ref[0, k]) + nn(pm_ref[1], x_ref[1, k])
        wgt = nn(cb_ref[...], corr, HI)
        ch, cl = splt(corr)
        wh, wl = splt(wgt)
        R[k, 0:256, :] = x_ref[0, k]
        R[k, 256:512, :] = x_ref[1, k]
        R[k, 512:576, :] = ch
        R[k, 576:640, :] = cl
        R[k, 640:704, :] = ch
        lt = jnp.concatenate([x_ref[0, k].astype(F32) * scale, x_ref[1, k].astype(F32) * scale,
                              wh.astype(F32), wh.astype(F32), wl.astype(F32)], axis=0)
        L[k] = lt.T.astype(BF)

    def block(t, _):
        g = nn(L[p_tab[t]], R[q_tab[t]]).astype(XDT)
        at = pl.multiple_of(t * 512, 512)
        o_ref[pl.ds(at, 256), :] = g[:, 0:128]
        o_ref[pl.ds(at + 256, 256), :] = g[:, 128:256]
        return 0
    lax.fori_loop(0, 18, block, 0)


def gram(p_tab, q_tab, x, pm, cb):
    vm = pl.BlockSpec(memory_space=pltpu.VMEM)
    sm = pl.BlockSpec(memory_space=pltpu.SMEM)
    return pl.pallas_call(
        gram_kernel, out_shape=jax.ShapeDtypeStruct((9216, 128), XDT),
        in_specs=[sm, sm, vm, vm, vm], out_specs=vm,
        scratch_shapes=[pltpu.VMEM((8, 256, 704), BF), pltpu.VMEM((8, 704, 256), BF)],
        compiler_params=pltpu.CompilerParams(vmem_limit_bytes=40 * 2**20))(p_tab, q_tab, x, pm, cb)


def sum_kernel(p_ref, o_ref, r1, r2, r3, s1, s2, ssem, rsem, fsem, gsem):
    band, grid = lax.axis_index("band"), lax.axis_index("grid")
    x, core = lax.div(band, 2), lax.rem(band, 2)
    z, y = lax.div(grid, 4), lax.rem(grid, 4)
    at = {"x": x, "y": y, "z": z}

    def peer(axis, d):
        to = lax.rem(at[axis] + d, 4)
        return {"x": {"band": 2 * to + core}, "y": {"grid": 4 * z + to}, "z": {"grid": 4 * to + y}}[axis]

    orders = ("xyz", "yzx", "zxy")
    mate = {"band": band + 1 - 2 * core}
    barrier([peer(a, d) for a in "xyz" for d in (1, 2, 3)] + [mate])

    def rows(start, n):
        return pl.ds(pl.multiple_of(start, 16), n)

    pend = []

    def send(stage, k, d, src, dst):
        i = (stage * 3 + k) * 3 + d - 1
        cp = pltpu.make_async_remote_copy(
            src_ref=src, dst_ref=dst, send_sem=ssem.at[i], recv_sem=rsem.at[i],
            device_id=peer(orders[k][stage if stage < 3 else 5 - stage], d), device_id_type=MESH)
        cp.start()
        pend.append(cp)
        return cp

    live = {}
    for d in (2, 1, 3):
        for k in range(3):
            a = lax.rem(at[orders[k][0]] + d, 4)
            live[k, d] = send(0, k, d, p_ref.at[rows(k * 3072 + a * 768, 768), :], r1.at[k, d - 1])
    for k in range(3):
        for d in (1, 3, 2):
            live[k, d].wait_recv()
        a = at[orders[k][0]]
        tot = p_ref[rows(k * 3072 + a * 768, 768), :].astype(F32)
        for d in range(3):
            tot = tot + r1[k, d].astype(F32)
        s1[k] = tot.astype(XDT)
        for d in (2, 1, 3):
            b = lax.rem(at[orders[k][1]] + d, 4)
            live[k, d] = send(1, k, d, s1.at[k, rows(b * 192, 192), :], r2.at[k, d - 1])
    for k in range(3):
        for d in (1, 3, 2):
            live[k, d].wait_recv()
        b = at[orders[k][1]]
        tot = s1[k, rows(b * 192, 192), :].astype(F32)
        for d in range(3):
            tot = tot + r2[k, d].astype(F32)
        s2[k] = tot.astype(XDT)
        for d in (2, 1, 3):
            c = lax.rem(at[orders[k][2]] + d, 4)
            live[k, d] = send(2, k, d, s2.at[k, rows(c * 48, 48), :], r3.at[k, d - 1])
    base = {}
    for k in range(3):
        for d in (1, 3, 2):
            live[k, d].wait_recv()
        a, b, c = (at[v] for v in orders[k])
        tot = s2[k, rows(c * 48, 48), :].astype(F32)
        for d in range(3):
            tot = tot + r3[k, d].astype(F32)
        base[k] = (k * 3072 + a * 768, b * 192, c * 48)
        here = o_ref.at[core, rows(sum(base[k]), 48), :]
        o_ref[core, rows(sum(base[k]), 48), :] = tot.astype(XDT)
        for d in (2, 1, 3):
            live[k, d] = send(3, k, d, here, here)
    for k in range(3):
        for d in (1, 3, 2):
            live[k, d].wait_recv()
        here = o_ref.at[core, rows(base[k][0] + base[k][1], 192), :]
        for d in (2, 1, 3):
            live[k, d] = send(4, k, d, here, here)
    fwd = []

    def forward(k, d, a):
        blk = o_ref.at[core, rows(k * 3072 + a * 768, 768), :]
        cp = pltpu.make_async_remote_copy(
            src_ref=blk, dst_ref=blk, send_sem=fsem.at[k * 4 + d], recv_sem=gsem.at[k * 4 + d],
            device_id=mate, device_id_type=MESH)
        cp.start()
        fwd.append(cp)

    for k in range(3):
        for d in (1, 3, 2):
            live[k, d].wait_recv()
        here = o_ref.at[core, rows(base[k][0], 768), :]
        for d in (2, 1, 3):
            live[k, d] = send(5, k, d, here, here)
        forward(k, 0, at[orders[k][0]])
    for d in (1, 3, 2):
        for k in range(3):
            live[k, d].wait_recv()
            forward(k, d, lax.rem(at[orders[k][0]] + 4 - d, 4))
    for cp in fwd:
        cp.wait()
    for cp in pend:
        cp.wait_send()


def total(part):
    vm = pl.BlockSpec(memory_space=pltpu.VMEM)
    return pl.pallas_call(
        sum_kernel, out_shape=jax.ShapeDtypeStruct((2, 9216, 128), XDT),
        in_specs=[vm], out_specs=vm,
        scratch_shapes=[pltpu.VMEM((3, 3, 768, 128), XDT), pltpu.VMEM((3, 3, 192, 128), XDT),
                        pltpu.VMEM((3, 3, 48, 128), XDT), pltpu.VMEM((3, 768, 128), XDT),
                        pltpu.VMEM((3, 192, 128), XDT),
                        pltpu.SemaphoreType.DMA((54,)), pltpu.SemaphoreType.DMA((54,)),
                        pltpu.SemaphoreType.DMA((12,)), pltpu.SemaphoreType.DMA((12,))],
        compiler_params=pltpu.CompilerParams(collective_id=1, has_side_effects=True,
                                             vmem_limit_bytes=40 * 2**20))(part)


def shards(orbitals, projectors, sphere_start, proj_count, owner_slab, correlation_coef):
    band = lax.axis_index("band")
    slab = lax.axis_index("grid")
    chip, core = band // 2, band % 2
    atoms = owner_slab.shape[0]
    mask = owner_slab == slab
    ids = jnp.arange(atoms, dtype=jnp.int32)
    rank = jnp.sum((ids[None, :] < ids[:, None]) & mask[None, :], axis=1, dtype=jnp.int32)
    pick = mask[None, :] & (rank[None, :] == jnp.arange(A_SLAB, dtype=jnp.int32)[:, None])
    starts = jnp.sum(jnp.where(pick, sphere_start[None, :], 0), axis=1)
    counts = jnp.sum(jnp.where(pick, proj_count[None, :], 0), axis=1)
    weights = jnp.dot(pick.astype(BF), projectors.reshape(atoms, NPMAX * SPH), preferred_element_type=F32)
    coefs = jnp.dot(pick.astype(F32), correlation_coef.reshape(atoms, NPMAX * NPMAX), precision=HI)
    active = jnp.arange(NPMAX, dtype=jnp.int32)[None, :] < counts[:, None]
    weights = jnp.where(active[:, :, None], weights.reshape(A_SLAB, NPMAX, SPH), 0.0).reshape(64, SPH)
    place = jnp.repeat(starts // SPH - chip * 4, NPMAX)
    pm = jnp.where(place[None, :, None, None] == jnp.arange(4, dtype=jnp.int32).reshape(2, 1, 2, 1),
                   weights[None, :, None, :], 0.0).reshape(2, 64, 256).astype(BF)
    eye = jnp.eye(A_SLAB, dtype=F32)
    cb = (eye[:, None, :, None] * coefs.reshape(A_SLAB, NPMAX, 1, NPMAX)).reshape(64, 64)
    p_all = jnp.asarray([p for p, _ in PAIRS], jnp.int32).reshape(2, 18)
    q_all = jnp.asarray([q for _, q in PAIRS], jnp.int32).reshape(2, 18)
    p_tab = jnp.where(core == 0, p_all[0], p_all[1])
    q_tab = jnp.where(core == 0, q_all[0], q_all[1])
    rows = swap(orbitals)
    part = gram(p_tab, q_tab, rows, pm, cb)
    metric = total(part)
    return factor_rotate(core, metric, rows)


def solution(mesh):
    in_specs = (P("grid", "band"), P(), P(), P(), P(), P())
    out_specs = P(("grid", "band"), None)
    return jax.shard_map(shards, mesh=mesh, in_specs=in_specs, out_specs=out_specs, check_vma=False)
```
